256 devices in a mesh: beam: 4 (over x, y), tm: 32 (over z), sub: 2 (over core).
Axes of the slice: x: 2, y: 2, z: 32, core: 2. Of those that a mesh axis runs over, the one named last changes fastest.
The devices are a block of a 4x8x32 slice.
Arguments:
- channels: bfloat16 [2, 8192, 4096], P(None, ('beam', 'tm'), 'sub'), parts along dimension 1, may hold values from -6 to 6
- synth_taps: float32 [4, 2, 2048], P(None, 'sub'), may hold values from 0.2 to 1
- chirp_phase: float32 [2048, 4096], P('tm', 'sub'), may hold values from -3.140625 to 3.140625
Outputs:
- dedispersed: float32 [2, 8192, 2, 2048], P(None, ('beam', 'tm'), 'sub'), parts along dimension 1
The draws below stay inside these ranges and needn't reach their ends.
There are 4 independent parts, one for each index of `beam`. The reference program is written for one: setup_inputs(seed, part) draws one part's arguments, and reference() takes and returns one part's arrays. A program takes and returns all parts, laid end to end along the dimension named above; an argument that names none is the same for every part. Nothing has to cross between parts.
All inputs are finite; a program needn't handle non-finite values.
Results may differ from the reference program's by a relative error of at most 0.0003.
Values may be sent and summed in bfloat16 or wider, within the bound.
A program may use at most 64 MiB of HBM per device.

```python
import math
import jax
import jax.numpy as jnp

C = 4096
P_SIZE = 4
FRAMES = 2048


def steps_of(stream_key, dims, shards, low, high):
    factor_of, own = 1.0, jax.random.fold_in(stream_key, 6)
    for position, blocks in shards:
        draws = jnp.exp(jax.random.uniform(jax.random.fold_in(own, position), (blocks,), jnp.float32, low / len(shards), high / len(shards)))
        factor_of = factor_of * jnp.repeat(draws, dims[position] // blocks).reshape([-1 if axis == position else 1 for axis in range(len(dims))])
    return factor_of


def bell_draw(key, extent, spread, bound, split=(), kind=jnp.bfloat16):
    loudness = steps_of(key, extent, split, -0.22, 0.18) if split else 1.0
    values = jax.random.normal(key, extent, jnp.float32) * spread * loudness
    return jnp.minimum(jnp.maximum(values, -bound), bound).astype(kind)


def setup_inputs(seed: int = 0, part: int = 0) -> dict:
    splits = jax.random.split(jax.random.key(seed), 4)
    part_keys = jax.random.split(jax.random.fold_in(splits[3], part), 4)
    return {
        "channels": bell_draw(part_keys[0], (2, FRAMES, C), 1.0, 6.0, ((1, 32), (2, 2))),
        "synth_taps": jnp.clip(0.2 + 0.8 * jax.random.uniform(splits[1], (P_SIZE, 2, C // 2), jnp.float32) ** steps_of(splits[1], (P_SIZE, 2, C // 2), ((1, 2),), -0.2, 0.2), 0.2, 1.0),
        "chirp_phase": jnp.clip(jax.random.uniform(splits[2], (FRAMES, C), jnp.float32, -3.140625, 3.140625), -3.140625, 3.140625),
    }


def reference(channels, synth_taps, chirp_phase):
    frame_count = channels.shape[1]
    width = channels.shape[2]
    spectrum = channels[0].astype(jnp.float32) + 1j * channels[1].astype(jnp.float32)
    voltage = jnp.fft.ifft(spectrum, axis=1) * math.sqrt(width)
    full_taps = jnp.transpose(synth_taps, (0, 2, 1)).reshape(P_SIZE, width)
    synthesized = full_taps[0] * voltage
    for offset in range(1, P_SIZE):
        delayed = jnp.concatenate([jnp.zeros((offset, width), voltage.dtype), voltage[:frame_count - offset]], axis=0)
        synthesized = synthesized + full_taps[offset] * delayed
    series = synthesized.reshape(-1)
    response = jnp.exp(1j * jnp.transpose(chirp_phase).reshape(-1))
    filtered = jnp.fft.ifft(jnp.fft.fft(series) * response).reshape(frame_count, width // 2, 2)
    filtered = jnp.transpose(filtered, (0, 2, 1))
    return jnp.stack([jnp.real(filtered), jnp.imag(filtered)]).astype(jnp.float32)
```

```python
import functools
import math

import jax
import jax.numpy as jnp
import numpy as np
from jax import lax
from jax.experimental import pallas as pl
from jax.experimental.pallas import tpu as pltpu
from jax.sharding import PartitionSpec as P

MESH = pl.DeviceIdType.MESH
f32 = jnp.float32
bf16 = jnp.bfloat16

WIDTH = 64
LANES = 2 * WIDTH
SUB = 8

SPAN = 160.0
BASE = SPAN / 2
FLOOR = 1e-35


def halves():
    lane = lax.broadcasted_iota(jnp.int32, (1, LANES), 1)
    return jnp.where(lane < WIDTH, -1.0, 1.0).astype(f32)


def swap(x):
    return pltpu.roll(x, WIDTH, x.ndim - 1)


def turned(x, table, conj=False):
    re, im = table
    return x * re - swap(x) * im if conj else x * re + swap(x) * im


def split(x):
    hi = x.astype(bf16)
    return hi, (x - hi.astype(f32)).astype(bf16)


def dot(a, b):
    return lax.dot_general(a, b, (((1,), (0,)), ((), ())), preferred_element_type=f32)


def left(matrix, blocks, conj):
    hi_ref, lo_ref = matrix
    sign = -halves() if conj else halves()
    tall = [jnp.concatenate([x, swap(x) * sign], axis=0) for x in blocks]
    hi, lo = split(jnp.concatenate(tall, axis=1))
    w_hi, w_lo = hi_ref[...], lo_ref[...]
    out = dot(w_hi, hi) + (dot(w_hi, lo) + dot(w_lo, hi))
    return [out[:, i * LANES : (i + 1) * LANES] for i in range(len(blocks))]


def right(matrix, x):
    hi_ref, lo_ref = matrix
    hi, lo = split(x)
    w_hi, w_lo = hi_ref[...], lo_ref[...]
    return dot(hi, w_hi) + (dot(lo, w_hi) + dot(hi, w_lo))


def encode(x, norm):
    top = jnp.maximum(jnp.max(jnp.abs(x), axis=0, keepdims=True), FLOOR)
    size = jnp.exp(jnp.abs(x) * (SPAN / top) - BASE)
    return jnp.where(x < 0, -size, size).astype(bf16), top * (norm / SPAN)


def decode(code, scale):
    code = code.astype(f32)
    size = jnp.log(jnp.abs(code)) + BASE
    return jnp.where(code < 0, -size, size) * scale


def circle(x):
    turns = jnp.floor(4.0 * x + 0.5)
    y = (2.0 * math.pi) * (x - 0.25 * turns)
    y2 = y * y
    sin = y * (1.0 + y2 * (-1.0 / 6 + y2 * (1.0 / 120 + y2 * (-1.0 / 5040 + y2 * (1.0 / 362880)))))
    cos = 1.0 + y2 * (-0.5 + y2 * (1.0 / 24 + y2 * (-1.0 / 720 + y2 * (1.0 / 40320))))
    quarter = turns - 4.0 * jnp.floor(0.25 * turns)
    odd = (quarter == 1.0) | (quarter == 3.0)
    flip_cos = (quarter == 1.0) | (quarter == 2.0)
    flip_sin = quarter >= 2.0
    first, second = jnp.where(odd, sin, cos), jnp.where(odd, cos, sin)
    return jnp.where(flip_cos, -first, first), jnp.where(flip_sin, -second, second)


def route(i, n):
    return n // 2 + (i + 1) // 2 * (2 * lax.rem(i, 2) - 1)


def beam_kernel(norm_in, norm_out, own, other, taps, phase_ref, turns_re, turns_im, twist_re, twist_im, long_hi, long_lo,
                inner_hi, inner_lo, outer_hi, outer_lo, plus_hi, plus_lo, minus_hi, minus_lo, out_ref, x_ref, v_ref, u_ref,
                z_ref, line_ref, t1_re, t1_im, t2_re, t2_im, resp_re, resp_im, mine_ref, theirs_ref, put, put_scale, got,
                got_scale, sent, arrived, sent_scale, arrived_scale, half_sent, half_arrived):
    n, rows, _ = x_ref.shape
    radix, length, _ = u_ref.shape
    step = length // radix
    chunks = rows // (2 * SUB)
    me = lax.axis_index("tm")
    parity = lax.axis_index("sub")
    long_m, inner_m, outer_m = (long_hi, long_lo), (inner_hi, inner_lo), (outer_hi, outer_lo)
    plus_m, minus_m = (plus_hi, plus_lo), (minus_hi, minus_lo)
    turn_re, turn_im = turns_re.at[parity], turns_im.at[parity]
    sign = 1.0 - 2.0 * parity.astype(f32)

    barrier = pltpu.get_barrier_semaphore()

    def greet(i, carry):
        peer = lax.rem(me + route(i, n), n)
        pl.semaphore_signal(barrier, inc=1, device_id={"tm": peer}, device_id_type=MESH)
        return carry

    lax.fori_loop(0, n - 1, greet, 0)
    pl.semaphore_signal(barrier, inc=1, device_id={"sub": 1 - parity}, device_id_type=MESH)

    def copies(phase, i, peer, slot):
        pairs = ((put_scale, got_scale, sent_scale, arrived_scale), (put, got, sent, arrived))
        return [
            pltpu.make_async_remote_copy(
                src_ref=source.at[phase, peer],
                dst_ref=target.at[phase, slot],
                send_sem=out_sem.at[phase, i],
                recv_sem=in_sem.at[phase, i],
                device_id={"tm": peer},
                device_id_type=MESH,
            )
            for source, target, out_sem, in_sem in pairs
        ]

    def send_all(phase, held, norm):

        def send(i, carry):
            peer = lax.rem(me + route(i, n), n)
            put[phase, peer], put_scale[phase, peer] = encode(held(peer), norm)
            for copy in copies(phase, i, peer, me):
                copy.start()
            return carry

        lax.fori_loop(0, n - 1, send, 0)
        got[phase, me], got_scale[phase, me] = encode(held(me), norm)

    def receive_all(phase, use):
        use(me, decode(got[phase, me], got_scale[phase, me]))

        def receive(i, carry):
            d = route(i, n)
            source = lax.rem(me + n - d, n)
            for copy in copies(phase, i, lax.rem(me + d, n), source):
                copy.wait_recv()
            use(source, decode(got[phase, source], got_scale[phase, source]))
            return carry

        lax.fori_loop(0, n - 1, receive, 0)

    def pair_of(c):
        return [pl.ds(pl.multiple_of((2 * c + i) * SUB, SUB), SUB) for i in range(2)]

    def across(c, blocks, conj):
        return [y.reshape(n, SUB, LANES) for y in left(long_m, [x.reshape(n * SUB, LANES) for x in blocks], conj)]

    def row_out(t):
        return right(plus_m, turned(v_ref[t], (twist_re[t], twist_im[t])))

    low = lax.broadcasted_iota(jnp.int32, (1, LANES), 1) < WIDTH
    for j in range(n // 2):
        cols = slice(j * LANES, (j + 1) * LANES)
        re = other[0, :, cols].astype(f32) + sign * own[0, :, cols].astype(f32)
        im = other[1, :, cols].astype(f32) + sign * own[1, :, cols].astype(f32)
        even = jnp.where(low, re, swap(im))
        odd = jnp.where(low, swap(re), im)
        x_ref[2 * j] = turned(even, (turn_re[2 * j], turn_im[2 * j]))
        x_ref[2 * j + 1] = turned(odd, (turn_re[2 * j + 1], turn_im[2 * j + 1]))

    def first_rows(c, carry):
        parts = pair_of(c)
        for part, y in zip(parts, across(c, [x_ref[:, part, :] for part in parts], True)):
            v_ref[:, part, :] = y
        return carry

    lax.fori_loop(0, chunks, first_rows, 0)
    pl.semaphore_wait(barrier, n)
    send_all(0, row_out, norm_in)

    lane = lax.broadcasted_iota(jnp.int32, (1, LANES), 1)
    row = lax.broadcasted_iota(jnp.int32, (length, 1), 0)
    column = 2 * (n * lax.rem(lane, WIDTH) + me) + parity
    frames = radix * length
    series_len = frames * 2 * WIDTH * n

    def column_tables(q, carry):
        cos, sin = circle((q * row).astype(f32) * (-1.0 / frames) + jnp.zeros((1, LANES), f32))
        t1_re[q], t1_im[q] = cos, sin * halves()
        cos, sin = circle(((q + radix * row) * column).astype(f32) * (-1.0 / series_len))
        t2_re[q], t2_im[q] = cos, sin * halves()
        return carry

    lax.fori_loop(0, radix, column_tables, 0)

    for j in range(n // 2):
        cos, sin = circle(phase_ref[:, j * LANES : (j + 1) * LANES] * (0.5 / math.pi))
        line_ref[2 * j * rows : (2 * j + 1) * rows] = cos
        line_ref[(2 * j + 1) * rows : (2 * j + 2) * rows] = sin
    for j in range(n // 2):
        for q in range(radix):
            part = slice(q * SUB, (q + 1) * SUB)
            cos = line_ref[pl.ds(2 * j * rows + q, SUB, stride=rows // SUB)]
            sin = line_ref[pl.ds((2 * j + 1) * rows + q, SUB, stride=rows // SUB)]
            far_cos, far_sin = swap(cos), swap(sin)
            resp_re[2 * j, part], resp_im[2 * j, part] = jnp.where(low, cos, far_cos), jnp.where(low, -sin, far_sin)
            resp_re[2 * j + 1, part] = jnp.where(low, far_cos, cos)
            resp_im[2 * j + 1, part] = jnp.where(low, -far_sin, sin)

    line_ref[0:SUB] = jnp.zeros((SUB, LANES), f32)

    def to_line(t, x):
        line_ref[pl.ds(pl.multiple_of(SUB + t * rows, SUB), rows)] = x

    receive_all(0, to_line)

    def filtered(start):
        window = line_ref[pl.ds(pl.multiple_of(start, SUB), SUB + step)]
        total = taps[0:1] * window[SUB:]
        for p in range(1, taps.shape[0]):
            total = total + taps[p : p + 1] * window[SUB - p : SUB - p + step]
        return total

    def starts_of(pair):
        return [pl.multiple_of((2 * pair + i) * step, step) for i in range(2)]

    def outer_in(pair, carry):
        starts = starts_of(pair)
        tall = [jnp.concatenate([filtered(a * length + start) for a in range(radix)], axis=0) for start in starts]
        for start, y in zip(starts, left(outer_m, tall, False)):
            part = pl.ds(start, step)
            u_ref[:, part, :] = turned(y.reshape(radix, step, LANES), (t1_re[:, part, :], t1_im[:, part, :]))
        return carry

    lax.fori_loop(0, radix // 2, outer_in, 0)

    def inner_in(pair, carry):
        for i, y in enumerate(left(inner_m, [u_ref[2 * pair], u_ref[2 * pair + 1]], False)):
            z_ref[2 * pair + i] = turned(y, (t2_re[2 * pair + i], t2_im[2 * pair + i]))
        return carry

    lax.fori_loop(0, radix // 2, inner_in, 0)

    def bins_of(t):
        return pl.ds(pl.multiple_of(t * SUB, SUB), SUB)

    send_all(1, lambda t: z_ref[:, bins_of(t), :].reshape(rows, LANES), 1.0)

    def row_in(t, x):
        x_ref[t] = turned(right(minus_m, x), (twist_re[t], twist_im[t]), True)

    receive_all(1, row_in)

    def half_copy(trip, c):
        part = pl.ds(pl.multiple_of(2 * c * SUB, 2 * SUB), 2 * SUB)
        return pltpu.make_async_remote_copy(
            src_ref=mine_ref.at[trip, :, part, :],
            dst_ref=theirs_ref.at[trip, :, part, :],
            send_sem=half_sent.at[trip, c],
            recv_sem=half_arrived.at[trip, c],
            device_id={"sub": 1 - parity},
            device_id_type=MESH,
        )

    def rows_forward(c, carry):
        parts = pair_of(c)
        for part, y in zip(parts, across(c, [x_ref[:, part, :] for part in parts], False)):
            mine_ref[0, :, part, :] = turned(y, (turn_re[...], turn_im[...]), True)
        half_copy(0, c).start()
        return carry

    lax.fori_loop(0, chunks, rows_forward, 0)

    def respond(c, carry):
        half_copy(0, c).wait_recv()
        for part in pair_of(c):
            both = theirs_ref[0, :, part, :] + sign * mine_ref[0, :, part, :]
            mine_ref[1, :, part, :] = turned(both, (resp_re[:, part, :], resp_im[:, part, :]))
        half_copy(1, c).start()
        return carry

    lax.fori_loop(0, chunks, respond, 0)

    def rows_back(c, carry):
        half_copy(1, c).wait_recv()
        parts = pair_of(c)
        both = [theirs_ref[1, :, part, :] + sign * mine_ref[1, :, part, :] for part in parts]
        for part, y in zip(parts, across(c, [turned(x, (turn_re[...], turn_im[...])) for x in both], True)):
            v_ref[:, part, :] = y
        return carry

    lax.fori_loop(0, chunks, rows_back, 0)
    send_all(2, row_out, 1.0)

    def to_bins(t, x):
        z_ref[:, bins_of(t), :] = x.reshape(radix, SUB, LANES)

    receive_all(2, to_bins)

    def inner_out(pair, carry):
        qs = (2 * pair, 2 * pair + 1)
        for q, y in zip(qs, left(inner_m, [turned(z_ref[q], (t2_re[q], t2_im[q]), True) for q in qs], True)):
            u_ref[q] = turned(y, (t1_re[q], t1_im[q]), True)
        return carry

    lax.fori_loop(0, radix // 2, inner_out, 0)

    def outer_out(pair, carry):
        starts = starts_of(pair)
        got_back = left(outer_m, [u_ref[:, pl.ds(start, step), :].reshape(length, LANES) for start in starts], True)
        for start, y in zip(starts, got_back):
            for a in range(radix):
                line_ref[pl.ds(pl.multiple_of(a * length + start, step), step)] = y[a * step : (a + 1) * step]
        return carry

    lax.fori_loop(0, radix // 2, outer_out, 0)
    send_all(3, lambda t: line_ref[pl.ds(pl.multiple_of(t * rows, SUB), rows)], norm_out)

    def to_out(t, x):
        out_ref[t] = x

    receive_all(3, to_out)

    def finish(i, carry):
        peer = lax.rem(me + route(i, n), n)
        for phase in range(4):
            for copy in copies(phase, i, peer, me):
                copy.wait_send()
        return carry

    lax.fori_loop(0, n - 1, finish, 0)

    def finish_halves(c, carry):
        for trip in range(2):
            half_copy(trip, c).wait_send()
        return carry

    lax.fori_loop(0, chunks, finish_halves, 0)


def as_parts(matrix):
    hi = matrix.astype(bf16)
    lo = (matrix - hi.astype(np.float64)).astype(bf16)
    return jnp.asarray(hi), jnp.asarray(lo)


def roots(left_count, right_count, length, direction):
    product = np.arange(left_count)[:, None] * np.arange(right_count)[None, :] % length
    return np.exp(direction * 2j * np.pi * product / length)


def left_parts(length, copies):
    full = np.kron(roots(length, length, length, -1), np.eye(copies))
    return as_parts(np.concatenate([full.real, full.imag], axis=1))


def right_parts(length, direction):
    full = roots(length, length, length, direction)
    return as_parts(np.block([[full.real, full.imag], [-full.imag, full.real]]))


def lane_table(values):
    re, im = values.real, values.imag
    return (
        jnp.asarray(np.concatenate([re, re], axis=-1), f32),
        jnp.asarray(np.concatenate([-im, im], axis=-1), f32),
    )


def body(channels, synth_taps, chirp_phase):
    frames_dev, half = channels.shape[1:]
    n = lax.axis_size("tm")
    me = lax.axis_index("tm")
    parity = lax.axis_index("sub")
    frames = frames_dev * n
    series_len = frames * 2 * half
    radix, length = SUB, frames // SUB
    tap_count = synth_taps.shape[0]

    def partner(x):
        size = lax.axis_size("sub")
        return lax.ppermute(x, "sub", [(i, size - 1 - i) for i in range(size)])

    long_m = left_parts(n, SUB)
    outer_m = left_parts(radix, length // radix)
    inner_m = left_parts(length, 1)
    short_plus, short_minus = right_parts(WIDTH, 1), right_parts(WIDTH, -1)

    twist = lane_table(roots(n, WIDTH, half, 1)[:, None, :])
    turn = np.exp(1j * np.pi * np.arange(half) / half).reshape(n, 1, WIDTH)
    turns = lane_table(np.stack([np.ones_like(turn), turn]))
    taps = lax.dynamic_index_in_dim(synth_taps.reshape(tap_count, WIDTH, n), me, 2, keepdims=False)
    taps = jnp.concatenate([taps, taps], axis=-1)
    args = (
        channels, partner(channels), taps, chirp_phase, *turns, *twist, *long_m, *inner_m, *outer_m, *short_plus,
        *short_minus,
    )
    grid_shape, tower = (n, frames_dev, LANES), (radix, length, LANES)
    phases = 4
    out = pl.pallas_call(
        functools.partial(beam_kernel, 1.0 / math.sqrt(2 * half), 1.0 / series_len),
        out_shape=jax.ShapeDtypeStruct(grid_shape, f32),
        in_specs=[pl.BlockSpec(memory_space=pltpu.VMEM)] * len(args),
        out_specs=pl.BlockSpec(memory_space=pltpu.VMEM),
        scratch_shapes=[
            pltpu.VMEM(grid_shape, f32),
            pltpu.VMEM(grid_shape, f32),
            pltpu.VMEM(tower, f32),
            pltpu.VMEM(tower, f32),
            pltpu.VMEM((SUB + frames, LANES), f32),
            *[pltpu.VMEM(tower, f32)] * 4,
            *[pltpu.VMEM(grid_shape, f32)] * 2,
            pltpu.VMEM((2, *grid_shape), f32),
            pltpu.VMEM((2, *grid_shape), f32),
            pltpu.VMEM((phases, *grid_shape), bf16),
            pltpu.VMEM((phases, n, 1, LANES), f32),
            pltpu.VMEM((phases, *grid_shape), bf16),
            pltpu.VMEM((phases, n, 1, LANES), f32),
            *[pltpu.SemaphoreType.DMA((phases, n))] * 4,
            *[pltpu.SemaphoreType.DMA((2, frames_dev // (2 * SUB)))] * 2,
        ],
        compiler_params=pltpu.CompilerParams(collective_id=1, has_side_effects=True, vmem_limit_bytes=56 * 2**20),
        name="beam",
    )(*args)
    out = out.reshape(n, frames_dev, 2, WIDTH).transpose(2, 1, 3, 0)
    return out.reshape(2, frames_dev, 1, half)


def solution(mesh):
    placed = (P(None, ("beam", "tm"), "sub"), P(None, "sub", None), P("tm", "sub"))
    return jax.shard_map(
        body,
        mesh=mesh,
        in_specs=placed,
        out_specs=P(None, ("beam", "tm"), "sub", None),
        check_vma=False,
    )
```

```python
import functools
import math

import jax
import jax.numpy as jnp
import numpy as np
from jax import lax
from jax.experimental import pallas as pl
from jax.experimental.pallas import tpu as pltpu
from jax.sharding import PartitionSpec as P

MESH = pl.DeviceIdType.MESH
f32 = jnp.float32
bf16 = jnp.bfloat16

WIDTH = 64
LANES = 2 * WIDTH
SUB = 8
GROUPS = 4

SPAN = 160.0
BASE = SPAN / 2
FLOOR = 1e-35


def halves():
    lane = lax.broadcasted_iota(jnp.int32, (1, LANES), 1)
    return jnp.where(lane < WIDTH, -1.0, 1.0).astype(f32)


def swap(x):
    return pltpu.roll(x, WIDTH, x.ndim - 1)


def turned(x, table, conj=False):
    re, im = table
    return x * re - swap(x) * im if conj else x * re + swap(x) * im


def split(x):
    hi = x.astype(bf16)
    return hi, (x - hi.astype(f32)).astype(bf16)


def dot(a, b):
    return lax.dot_general(a, b, (((1,), (0,)), ((), ())), preferred_element_type=f32)


def left(matrix, blocks, conj):
    hi_ref, lo_ref = matrix
    sign = -halves() if conj else halves()
    tall = [jnp.concatenate([x, swap(x) * sign], axis=0) for x in blocks]
    hi, lo = split(jnp.concatenate(tall, axis=1))
    w_hi, w_lo = hi_ref[...], lo_ref[...]
    out = dot(w_hi, hi) + (dot(w_hi, lo) + dot(w_lo, hi))
    return [out[:, i * LANES : (i + 1) * LANES] for i in range(len(blocks))]


def right(matrix, x):
    hi_ref, lo_ref = matrix
    hi, lo = split(x)
    w_hi, w_lo = hi_ref[...], lo_ref[...]
    return dot(hi, w_hi) + (dot(lo, w_hi) + dot(hi, w_lo))


def encode(x, norm):
    top = jnp.maximum(jnp.max(jnp.abs(x), axis=0, keepdims=True), FLOOR)
    size = jnp.exp(jnp.abs(x) * (SPAN / top) - BASE)
    return jnp.where(x < 0, -size, size).astype(bf16), top * (norm / SPAN)


def decode(code, scale):
    code = code.astype(f32)
    size = jnp.log(jnp.abs(code)) + BASE
    return jnp.where(code < 0, -size, size) * scale


def circle(x):
    turns = jnp.floor(4.0 * x + 0.5)
    y = (2.0 * math.pi) * (x - 0.25 * turns)
    y2 = y * y
    sin = y * (1.0 + y2 * (-1.0 / 6 + y2 * (1.0 / 120 + y2 * (-1.0 / 5040 + y2 * (1.0 / 362880)))))
    cos = 1.0 + y2 * (-0.5 + y2 * (1.0 / 24 + y2 * (-1.0 / 720 + y2 * (1.0 / 40320))))
    quarter = turns - 4.0 * jnp.floor(0.25 * turns)
    odd = (quarter == 1.0) | (quarter == 3.0)
    flip_cos = (quarter == 1.0) | (quarter == 2.0)
    flip_sin = quarter >= 2.0
    first, second = jnp.where(odd, sin, cos), jnp.where(odd, cos, sin)
    return jnp.where(flip_cos, -first, first), jnp.where(flip_sin, -second, second)


def route(i, n):
    return n // 2 + (i + 1) // 2 * (2 * lax.rem(i, 2) - 1)


def group_route(group, i, n):
    count = n // GROUPS
    return group + GROUPS * lax.rem(count // 2 + (i + 1) // 2 * (1 - 2 * lax.rem(i, 2)) + count, count)


def beam_kernel(norm_in, norm_out, own, other, taps, phase_ref, turns_re, turns_im, twist_re, twist_im, long_hi, long_lo,
                inner_hi, inner_lo, outer_hi, outer_lo, plus_hi, plus_lo, minus_hi, minus_lo, out_ref, x_ref, v_ref, u_ref,
                z_ref, line_ref, t1_re, t1_im, t2_re, t2_im, resp_re, resp_im, mine_ref, theirs_ref, put, put_scale, got,
                got_scale, sent, arrived, sent_scale, arrived_scale, half_sent, half_arrived):
    n, rows, _ = x_ref.shape
    radix, length, _ = u_ref.shape
    step = length // radix
    chunks = rows // (2 * SUB)
    me = lax.axis_index("tm")
    parity = lax.axis_index("sub")
    long_m, inner_m, outer_m = (long_hi, long_lo), (inner_hi, inner_lo), (outer_hi, outer_lo)
    plus_m, minus_m = (plus_hi, plus_lo), (minus_hi, minus_lo)
    turn_re, turn_im = turns_re.at[parity], turns_im.at[parity]
    sign = 1.0 - 2.0 * parity.astype(f32)

    barrier = pltpu.get_barrier_semaphore()

    def greet(i, carry):
        peer = lax.rem(me + route(i, n), n)
        pl.semaphore_signal(barrier, inc=1, device_id={"tm": peer}, device_id_type=MESH)
        return carry

    lax.fori_loop(0, n - 1, greet, 0)
    pl.semaphore_signal(barrier, inc=1, device_id={"sub": 1 - parity}, device_id_type=MESH)

    def copies(trip, d, count):
        peer = lax.rem(me + d, n)
        part = pl.ds(0, count)
        kinds = (
            (put_scale.at[trip, peer], got_scale.at[trip, me], sent_scale, arrived_scale),
            (put.at[trip, peer, part, :], got.at[trip, me, part, :], sent, arrived),
        )
        return [
            pltpu.make_async_remote_copy(
                src_ref=source,
                dst_ref=target,
                send_sem=out_sem.at[trip, d],
                recv_sem=in_sem.at[trip, d],
                device_id={"tm": peer},
                device_id_type=MESH,
            )
            for source, target, out_sem, in_sem in kinds
        ]

    def keep(trip, count, held, norm):
        got[trip, me, 0:count, :], got_scale[trip, me] = encode(held(me), norm)

    def send(trip, count, d, held, norm):
        peer = lax.rem(me + d, n)
        put[trip, peer, 0:count, :], put_scale[trip, peer] = encode(held(peer), norm)
        for copy in copies(trip, d, count):
            copy.start()

    def take(trip, count, d, use):
        source = lax.rem(me + n - d, n)
        for copy in copies(trip, d, count):
            copy.wait_recv()
        use(source, decode(got[trip, source, 0:count, :], got_scale[trip, source]))

    def take_own(trip, count, use):
        use(me, decode(got[trip, me, 0:count, :], got_scale[trip, me]))

    def each(count, act):

        def step_of(i, carry):
            act(i)
            return carry

        lax.fori_loop(0, count, step_of, 0)

    def send_all(trip, count, held, norm):
        each(n - 1, lambda i: send(trip, count, route(i, n), held, norm))
        keep(trip, count, held, norm)

    def take_all(trip, count, use):
        take_own(trip, count, use)
        each(n - 1, lambda i: take(trip, count, route(i, n), use))

    group_size = n // GROUPS

    def send_group(trip, group, held, norm):
        each(group_size - (group == 0), lambda i: send(trip, rows, group_route(group, i, n), held, norm))

    def take_group(trip, group, use):
        each(group_size - (group == 0), lambda i: take(trip, rows, group_route(group, i, n), use))

    def pair_of(c):
        return [pl.ds(pl.multiple_of((2 * c + i) * SUB, SUB), SUB) for i in range(2)]

    def across(c, blocks, conj):
        return [y.reshape(n, SUB, LANES) for y in left(long_m, [x.reshape(n * SUB, LANES) for x in blocks], conj)]

    def row_out(t, part=slice(None)):
        return right(plus_m, turned(v_ref[t, part, :], (twist_re[t], twist_im[t])))

    low = lax.broadcasted_iota(jnp.int32, (1, LANES), 1) < WIDTH
    for j in range(n // 2):
        cols = slice(j * LANES, (j + 1) * LANES)
        re = other[0, :, cols].astype(f32) + sign * own[0, :, cols].astype(f32)
        im = other[1, :, cols].astype(f32) + sign * own[1, :, cols].astype(f32)
        even = jnp.where(low, re, swap(im))
        odd = jnp.where(low, swap(re), im)
        x_ref[2 * j] = turned(even, (turn_re[2 * j], turn_im[2 * j]))
        x_ref[2 * j + 1] = turned(odd, (turn_re[2 * j + 1], turn_im[2 * j + 1]))

    def first_rows(c, carry):
        parts = pair_of(c)
        for part, y in zip(parts, across(c, [x_ref[:, part, :] for part in parts], True)):
            v_ref[:, part, :] = y
        return carry

    lax.fori_loop(0, chunks, first_rows, 0)
    pl.semaphore_wait(barrier, n)
    for group in range(GROUPS):
        send_group(0, group, row_out, norm_in)
    keep(0, rows, row_out, norm_in)

    lane = lax.broadcasted_iota(jnp.int32, (1, LANES), 1)
    row = lax.broadcasted_iota(jnp.int32, (length, 1), 0)
    column = 2 * (n * lax.rem(lane, WIDTH) + me) + parity
    frames = radix * length
    series_len = frames * 2 * WIDTH * n

    def column_tables(q, carry):
        cos, sin = circle((q * row).astype(f32) * (-1.0 / frames) + jnp.zeros((1, LANES), f32))
        t1_re[q], t1_im[q] = cos, sin * halves()
        cos, sin = circle(((q + radix * row) * column).astype(f32) * (-1.0 / series_len))
        t2_re[q], t2_im[q] = cos, sin * halves()
        return carry

    lax.fori_loop(0, radix, column_tables, 0)

    for j in range(n // 2):
        cos, sin = circle(phase_ref[:, j * LANES : (j + 1) * LANES] * (0.5 / math.pi))
        line_ref[2 * j * rows : (2 * j + 1) * rows] = cos
        line_ref[(2 * j + 1) * rows : (2 * j + 2) * rows] = sin
    for j in range(n // 2):
        for q in range(radix):
            part = slice(q * SUB, (q + 1) * SUB)
            cos = line_ref[pl.ds(2 * j * rows + q, SUB, stride=rows // SUB)]
            sin = line_ref[pl.ds((2 * j + 1) * rows + q, SUB, stride=rows // SUB)]
            far_cos, far_sin = swap(cos), swap(sin)
            resp_re[2 * j, part], resp_im[2 * j, part] = jnp.where(low, cos, far_cos), jnp.where(low, -sin, far_sin)
            resp_re[2 * j + 1, part] = jnp.where(low, far_cos, cos)
            resp_im[2 * j + 1, part] = jnp.where(low, -far_sin, sin)

    line_ref[0:SUB] = jnp.zeros((SUB, LANES), f32)

    def to_line(t, x):
        line_ref[pl.ds(pl.multiple_of(SUB + t * rows, SUB), rows)] = x

    def filtered(start):
        window = line_ref[pl.ds(pl.multiple_of(start, SUB), SUB + step)]
        total = taps[0:1] * window[SUB:]
        for p in range(1, taps.shape[0]):
            total = total + taps[p : p + 1] * window[SUB - p : SUB - p + step]
        return total

    def starts_of(pair):
        return [pl.multiple_of((2 * pair + i) * step, step) for i in range(2)]

    def outer_in(pair, carry):
        starts = starts_of(pair)
        tall = [jnp.concatenate([filtered(a * length + start) for a in range(radix)], axis=0) for start in starts]
        for start, y in zip(starts, left(outer_m, tall, False)):
            part = pl.ds(start, step)
            u_ref[:, part, :] = turned(y.reshape(radix, step, LANES), (t1_re[:, part, :], t1_im[:, part, :]))
        return carry

    take_own(0, rows, to_line)
    for group in range(GROUPS):
        take_group(0, group, to_line)
        if group:
            outer_in(lax.rem(me + n - group + 1, GROUPS), 0)
    outer_in(lax.rem(me + n - GROUPS + 1, GROUPS), 0)

    def inner_in(pair, carry):
        for i, y in enumerate(left(inner_m, [u_ref[2 * pair], u_ref[2 * pair + 1]], False)):
            z_ref[2 * pair + i] = turned(y, (t2_re[2 * pair + i], t2_im[2 * pair + i]))
        return carry

    def bins_of(t):
        return pl.ds(pl.multiple_of(t * SUB, SUB), SUB)

    half_rows, half_radix = rows // 2, radix // 2
    for h in range(2):
        lax.fori_loop(h * half_radix // 2, (h + 1) * half_radix // 2, inner_in, 0)
        towers = slice(h * half_radix, (h + 1) * half_radix)
        send_all(1 + h, half_rows, lambda t: z_ref[towers, bins_of(t), :].reshape(half_rows, LANES), 1.0)

    def half_copy(trip, c):
        part = pl.ds(pl.multiple_of(2 * c * SUB, 2 * SUB), 2 * SUB)
        return pltpu.make_async_remote_copy(
            src_ref=mine_ref.at[trip, :, part, :],
            dst_ref=theirs_ref.at[trip, :, part, :],
            send_sem=half_sent.at[trip, c],
            recv_sem=half_arrived.at[trip, c],
            device_id={"sub": 1 - parity},
            device_id_type=MESH,
        )

    def rows_forward(c, carry):
        parts = pair_of(c)
        for part, y in zip(parts, across(c, [x_ref[:, part, :] for part in parts], False)):
            mine_ref[0, :, part, :] = turned(y, (turn_re[...], turn_im[...]), True)
        half_copy(0, c).start()
        return carry

    def respond(c, carry):
        half_copy(0, c).wait_recv()
        for part in pair_of(c):
            both = theirs_ref[0, :, part, :] + sign * mine_ref[0, :, part, :]
            mine_ref[1, :, part, :] = turned(both, (resp_re[:, part, :], resp_im[:, part, :]))
        half_copy(1, c).start()
        return carry

    def rows_back(c, carry):
        half_copy(1, c).wait_recv()
        parts = pair_of(c)
        both = [theirs_ref[1, :, part, :] + sign * mine_ref[1, :, part, :] for part in parts]
        for part, y in zip(parts, across(c, [turned(x, (turn_re[...], turn_im[...])) for x in both], True)):
            v_ref[:, part, :] = y
        return carry

    for h in range(2):
        part = slice(h * half_rows, (h + 1) * half_rows)

        def row_in(t, x):
            x_ref[t, part, :] = turned(right(minus_m, x), (twist_re[t], twist_im[t]), True)

        take_all(1 + h, half_rows, row_in)
        for act in (rows_forward, respond, rows_back):
            lax.fori_loop(h * chunks // 2, (h + 1) * chunks // 2, act, 0)
        send_all(3 + h, half_rows, lambda t: row_out(t, part), 1.0)

    def inner_out(pair, carry):
        qs = (2 * pair, 2 * pair + 1)
        for q, y in zip(qs, left(inner_m, [turned(z_ref[q], (t2_re[q], t2_im[q]), True) for q in qs], True)):
            u_ref[q] = turned(y, (t1_re[q], t1_im[q]), True)
        return carry

    for h in range(2):
        towers = slice(h * half_radix, (h + 1) * half_radix)

        def to_bins(t, x):
            z_ref[towers, bins_of(t), :] = x.reshape(half_radix, SUB, LANES)

        take_all(3 + h, half_rows, to_bins)
        lax.fori_loop(h * half_radix // 2, (h + 1) * half_radix // 2, inner_out, 0)

    def outer_out(pair, carry):
        starts = starts_of(pair)
        got_back = left(outer_m, [u_ref[:, pl.ds(start, step), :].reshape(length, LANES) for start in starts], True)
        for start, y in zip(starts, got_back):
            for a in range(radix):
                line_ref[pl.ds(pl.multiple_of(a * length + start, step), step)] = y[a * step : (a + 1) * step]
        return carry

    def frames_of(t):
        return line_ref[pl.ds(pl.multiple_of(t * rows, SUB), rows)]

    for group in range(GROUPS):
        outer_out(lax.rem(me + group, GROUPS), 0)
        send_group(5, group, frames_of, norm_out)
    keep(5, rows, frames_of, norm_out)

    def to_out(t, x):
        out_ref[t] = x

    take_own(5, rows, to_out)
    for group in range(GROUPS):
        take_group(5, group, to_out)

    def finish(i):
        for trip, count in enumerate((rows, *[half_rows] * 4, rows)):
            for copy in copies(trip, i + 1, count):
                copy.wait_send()

    each(n - 1, finish)

    def finish_halves(c, carry):
        for trip in range(2):
            half_copy(trip, c).wait_send()
        return carry

    lax.fori_loop(0, chunks, finish_halves, 0)


def as_parts(matrix):
    hi = matrix.astype(bf16)
    lo = (matrix - hi.astype(np.float64)).astype(bf16)
    return jnp.asarray(hi), jnp.asarray(lo)


def roots(left_count, right_count, length, direction):
    product = np.arange(left_count)[:, None] * np.arange(right_count)[None, :] % length
    return np.exp(direction * 2j * np.pi * product / length)


def left_parts(length, copies):
    full = np.kron(roots(length, length, length, -1), np.eye(copies))
    return as_parts(np.concatenate([full.real, full.imag], axis=1))


def right_parts(length, direction):
    full = roots(length, length, length, direction)
    return as_parts(np.block([[full.real, full.imag], [-full.imag, full.real]]))


def lane_table(values):
    re, im = values.real, values.imag
    return (
        jnp.asarray(np.concatenate([re, re], axis=-1), f32),
        jnp.asarray(np.concatenate([-im, im], axis=-1), f32),
    )


def body(channels, synth_taps, chirp_phase):
    frames_dev, half = channels.shape[1:]
    n = lax.axis_size("tm")
    me = lax.axis_index("tm")
    parity = lax.axis_index("sub")
    frames = frames_dev * n
    series_len = frames * 2 * half
    radix, length = SUB, frames // SUB
    tap_count = synth_taps.shape[0]

    def partner(x):
        size = lax.axis_size("sub")
        return lax.ppermute(x, "sub", [(i, size - 1 - i) for i in range(size)])

    long_m = left_parts(n, SUB)
    outer_m = left_parts(radix, length // radix)
    inner_m = left_parts(length, 1)
    short_plus, short_minus = right_parts(WIDTH, 1), right_parts(WIDTH, -1)

    twist = lane_table(roots(n, WIDTH, half, 1)[:, None, :])
    turn = np.exp(1j * np.pi * np.arange(half) / half).reshape(n, 1, WIDTH)
    turns = lane_table(np.stack([np.ones_like(turn), turn]))
    taps = lax.dynamic_index_in_dim(synth_taps.reshape(tap_count, WIDTH, n), me, 2, keepdims=False)
    taps = jnp.concatenate([taps, taps], axis=-1)
    args = (
        channels, partner(channels), taps, chirp_phase, *turns, *twist, *long_m, *inner_m, *outer_m, *short_plus,
        *short_minus,
    )
    grid_shape, tower = (n, frames_dev, LANES), (radix, length, LANES)
    trips = 6
    out = pl.pallas_call(
        functools.partial(beam_kernel, 1.0 / math.sqrt(2 * half), 1.0 / series_len),
        out_shape=jax.ShapeDtypeStruct(grid_shape, f32),
        in_specs=[pl.BlockSpec(memory_space=pltpu.VMEM)] * len(args),
        out_specs=pl.BlockSpec(memory_space=pltpu.VMEM),
        scratch_shapes=[
            pltpu.VMEM(grid_shape, f32),
            pltpu.VMEM(grid_shape, f32),
            pltpu.VMEM(tower, f32),
            pltpu.VMEM(tower, f32),
            pltpu.VMEM((SUB + frames, LANES), f32),
            *[pltpu.VMEM(tower, f32)] * 4,
            *[pltpu.VMEM(grid_shape, f32)] * 2,
            pltpu.VMEM((2, *grid_shape), f32),
            pltpu.VMEM((2, *grid_shape), f32),
            pltpu.VMEM((trips, *grid_shape), bf16),
            pltpu.VMEM((trips, n, 1, LANES), f32),
            pltpu.VMEM((trips, *grid_shape), bf16),
            pltpu.VMEM((trips, n, 1, LANES), f32),
            *[pltpu.SemaphoreType.DMA((trips, n))] * 4,
            *[pltpu.SemaphoreType.DMA((2, frames_dev // (2 * SUB)))] * 2,
        ],
        compiler_params=pltpu.CompilerParams(collective_id=1, has_side_effects=True, vmem_limit_bytes=56 * 2**20),
        name="beam",
    )(*args)
    out = out.reshape(n, frames_dev, 2, WIDTH).transpose(2, 1, 3, 0)
    return out.reshape(2, frames_dev, 1, half)


def solution(mesh):
    placed = (P(None, ("beam", "tm"), "sub"), P(None, "sub", None), P("tm", "sub"))
    return jax.shard_map(
        body,
        mesh=mesh,
        in_specs=placed,
        out_specs=P(None, ("beam", "tm"), "sub", None),
        check_vma=False,
    )
```

```python
import functools
import math

import jax
import jax.numpy as jnp
import numpy as np
from jax import lax
from jax.experimental import pallas as pl
from jax.experimental.pallas import tpu as pltpu
from jax.sharding import PartitionSpec as P

MESH = pl.DeviceIdType.MESH
f32 = jnp.float32
bf16 = jnp.bfloat16

WIDTH = 64
LANES = 2 * WIDTH
SUB = 8
GROUPS = 4

SPAN = 160.0
BASE = SPAN / 2
FLOOR = 1e-35


def halves():
    lane = lax.broadcasted_iota(jnp.int32, (1, LANES), 1)
    return jnp.where(lane < WIDTH, -1.0, 1.0).astype(f32)


def swap(x):
    return pltpu.roll(x, WIDTH, x.ndim - 1)


def turned(x, table, conj=False):
    re, im = table
    return x * re - swap(x) * im if conj else x * re + swap(x) * im


def split(x):
    hi = x.astype(bf16)
    return hi, (x - hi.astype(f32)).astype(bf16)


def dot(a, b):
    return lax.dot_general(a, b, (((1,), (0,)), ((), ())), preferred_element_type=f32)


def left(matrix, blocks, conj):
    hi_ref, lo_ref = matrix
    sign = -halves() if conj else halves()
    tall = [jnp.concatenate([x, swap(x) * sign], axis=0) for x in blocks]
    hi, lo = split(jnp.concatenate(tall, axis=1))
    w_hi, w_lo = hi_ref[...], lo_ref[...]
    out = dot(w_hi, hi) + (dot(w_hi, lo) + dot(w_lo, hi))
    return [out[:, i * LANES : (i + 1) * LANES] for i in range(len(blocks))]


def right(matrix, x):
    hi_ref, lo_ref = matrix
    hi, lo = split(x)
    w_hi, w_lo = hi_ref[...], lo_ref[...]
    return dot(hi, w_hi) + (dot(lo, w_hi) + dot(hi, w_lo))


def encode(x, norm):
    top = jnp.maximum(jnp.max(jnp.abs(x), axis=0, keepdims=True), FLOOR)
    size = jnp.exp(jnp.abs(x) * (SPAN / top) - BASE)
    return jnp.where(x < 0, -size, size).astype(bf16), top * (norm / SPAN)


def decode(code, scale):
    code = code.astype(f32)
    size = jnp.log(jnp.abs(code)) + BASE
    return jnp.where(code < 0, -size, size) * scale


def circle(x):
    turns = jnp.floor(4.0 * x + 0.5)
    y = (2.0 * math.pi) * (x - 0.25 * turns)
    y2 = y * y
    sin = y * (1.0 + y2 * (-1.0 / 6 + y2 * (1.0 / 120 + y2 * (-1.0 / 5040 + y2 * (1.0 / 362880)))))
    cos = 1.0 + y2 * (-0.5 + y2 * (1.0 / 24 + y2 * (-1.0 / 720 + y2 * (1.0 / 40320))))
    quarter = turns - 4.0 * jnp.floor(0.25 * turns)
    odd = (quarter == 1.0) | (quarter == 3.0)
    flip_cos = (quarter == 1.0) | (quarter == 2.0)
    flip_sin = quarter >= 2.0
    first, second = jnp.where(odd, sin, cos), jnp.where(odd, cos, sin)
    return jnp.where(flip_cos, -first, first), jnp.where(flip_sin, -second, second)


def route(i, n):
    turn, near = lax.rem(i + 3, 4), (i + 3) // 4
    far, back = turn // 2, lax.rem(turn, 2)
    return far * (n // 2) + (1 - far) * back * n + (1 - 2 * back) * (1 - 2 * far) * near


def group_route(group, i, n):
    count = n // GROUPS
    return group + GROUPS * lax.rem(count // 2 + (i + 1) // 2 * (1 - 2 * lax.rem(i, 2)) + count, count)


def beam_kernel(norm_in, norm_out, own, other, taps, phase_ref, turns_re, turns_im, twist_re, twist_im, long_hi, long_lo,
                inner_hi, inner_lo, outer_hi, outer_lo, plus_hi, plus_lo, minus_hi, minus_lo, out_ref, x_ref, v_ref, u_ref,
                z_ref, line_ref, t1_re, t1_im, t2_re, t2_im, resp_re, resp_im, mine_ref, theirs_ref, put, put_scale, got,
                got_scale, sent, arrived, sent_scale, arrived_scale, half_sent, half_arrived):
    n, rows, _ = x_ref.shape
    radix, length, _ = u_ref.shape
    step = length // radix
    chunks = rows // (2 * SUB)
    me = lax.axis_index("tm")
    parity = lax.axis_index("sub")
    long_m, inner_m, outer_m = (long_hi, long_lo), (inner_hi, inner_lo), (outer_hi, outer_lo)
    plus_m, minus_m = (plus_hi, plus_lo), (minus_hi, minus_lo)
    turn_re, turn_im = turns_re.at[parity], turns_im.at[parity]
    sign = 1.0 - 2.0 * parity.astype(f32)

    barrier = pltpu.get_barrier_semaphore()

    def greet(i, carry):
        peer = lax.rem(me + route(i, n), n)
        pl.semaphore_signal(barrier, inc=1, device_id={"tm": peer}, device_id_type=MESH)
        return carry

    lax.fori_loop(0, n - 1, greet, 0)
    pl.semaphore_signal(barrier, inc=1, device_id={"sub": 1 - parity}, device_id_type=MESH)

    def copies(trip, d, count):
        peer = lax.rem(me + d, n)
        part = pl.ds(0, count)
        kinds = (
            (put_scale.at[trip, peer], got_scale.at[trip, me], sent_scale, arrived_scale),
            (put.at[trip, peer, part, :], got.at[trip, me, part, :], sent, arrived),
        )
        return [
            pltpu.make_async_remote_copy(
                src_ref=source,
                dst_ref=target,
                send_sem=out_sem.at[trip, d],
                recv_sem=in_sem.at[trip, d],
                device_id={"tm": peer},
                device_id_type=MESH,
            )
            for source, target, out_sem, in_sem in kinds
        ]

    def keep(trip, count, held, norm):
        got[trip, me, 0:count, :], got_scale[trip, me] = encode(held(me), norm)

    def send(trip, count, d, held, norm):
        peer = lax.rem(me + d, n)
        put[trip, peer, 0:count, :], put_scale[trip, peer] = encode(held(peer), norm)
        for copy in copies(trip, d, count):
            copy.start()

    def take(trip, count, d, use):
        source = lax.rem(me + n - d, n)
        for copy in copies(trip, d, count):
            copy.wait_recv()
        use(source, decode(got[trip, source, 0:count, :], got_scale[trip, source]))

    def take_own(trip, count, use):
        use(me, decode(got[trip, me, 0:count, :], got_scale[trip, me]))

    def each(count, act):

        def step_of(i, carry):
            act(i)
            return carry

        lax.fori_loop(0, count, step_of, 0)

    def send_all(trip, count, held, norm):
        each(n - 1, lambda i: send(trip, count, route(i, n), held, norm))
        keep(trip, count, held, norm)

    def take_all(trip, count, use):
        take_own(trip, count, use)
        each(n - 1, lambda i: take(trip, count, route(i, n), use))

    group_size = n // GROUPS

    def send_group(trip, group, held, norm):
        each(group_size - (group == 0), lambda i: send(trip, rows, group_route(group, i, n), held, norm))

    def take_group(trip, group, use):
        each(group_size - (group == 0), lambda i: take(trip, rows, group_route(group, i, n), use))

    def pair_of(c):
        return [pl.ds(pl.multiple_of((2 * c + i) * SUB, SUB), SUB) for i in range(2)]

    def across(c, blocks, conj):
        return [y.reshape(n, SUB, LANES) for y in left(long_m, [x.reshape(n * SUB, LANES) for x in blocks], conj)]

    def row_out(t, part=slice(None)):
        return right(plus_m, turned(v_ref[t, part, :], (twist_re[t], twist_im[t])))

    low = lax.broadcasted_iota(jnp.int32, (1, LANES), 1) < WIDTH
    for j in range(n // 2):
        cols = slice(j * LANES, (j + 1) * LANES)
        re = other[0, :, cols].astype(f32) + sign * own[0, :, cols].astype(f32)
        im = other[1, :, cols].astype(f32) + sign * own[1, :, cols].astype(f32)
        even = jnp.where(low, re, swap(im))
        odd = jnp.where(low, swap(re), im)
        x_ref[2 * j] = turned(even, (turn_re[2 * j], turn_im[2 * j]))
        x_ref[2 * j + 1] = turned(odd, (turn_re[2 * j + 1], turn_im[2 * j + 1]))

    def first_rows(c, carry):
        parts = pair_of(c)
        for part, y in zip(parts, across(c, [x_ref[:, part, :] for part in parts], True)):
            v_ref[:, part, :] = y
        return carry

    lax.fori_loop(0, chunks, first_rows, 0)
    pl.semaphore_wait(barrier, n)
    for group in range(GROUPS):
        send_group(0, group, row_out, norm_in)
    keep(0, rows, row_out, norm_in)

    lane = lax.broadcasted_iota(jnp.int32, (1, LANES), 1)
    row = lax.broadcasted_iota(jnp.int32, (length, 1), 0)
    column = 2 * (n * lax.rem(lane, WIDTH) + me) + parity
    frames = radix * length
    series_len = frames * 2 * WIDTH * n

    def column_tables(q, carry):
        cos, sin = circle((q * row).astype(f32) * (-1.0 / frames) + jnp.zeros((1, LANES), f32))
        t1_re[q], t1_im[q] = cos, sin * halves()
        cos, sin = circle(((q + radix * row) * column).astype(f32) * (-1.0 / series_len))
        t2_re[q], t2_im[q] = cos, sin * halves()
        return carry

    lax.fori_loop(0, radix, column_tables, 0)

    for j in range(n // 2):
        cos, sin = circle(phase_ref[:, j * LANES : (j + 1) * LANES] * (0.5 / math.pi))
        line_ref[2 * j * rows : (2 * j + 1) * rows] = cos
        line_ref[(2 * j + 1) * rows : (2 * j + 2) * rows] = sin
    for j in range(n // 2):
        for q in range(radix):
            part = slice(q * SUB, (q + 1) * SUB)
            cos = line_ref[pl.ds(2 * j * rows + q, SUB, stride=rows // SUB)]
            sin = line_ref[pl.ds((2 * j + 1) * rows + q, SUB, stride=rows // SUB)]
            far_cos, far_sin = swap(cos), swap(sin)
            resp_re[2 * j, part], resp_im[2 * j, part] = jnp.where(low, cos, far_cos), jnp.where(low, -sin, far_sin)
            resp_re[2 * j + 1, part] = jnp.where(low, far_cos, cos)
            resp_im[2 * j + 1, part] = jnp.where(low, -far_sin, sin)

    line_ref[0:SUB] = jnp.zeros((SUB, LANES), f32)

    def to_line(t, x):
        line_ref[pl.ds(pl.multiple_of(SUB + t * rows, SUB), rows)] = x

    def filtered(start):
        window = line_ref[pl.ds(pl.multiple_of(start, SUB), SUB + step)]
        total = taps[0:1] * window[SUB:]
        for p in range(1, taps.shape[0]):
            total = total + taps[p : p + 1] * window[SUB - p : SUB - p + step]
        return total

    def starts_of(pair):
        return [pl.multiple_of((2 * pair + i) * step, step) for i in range(2)]

    def outer_in(pair, carry):
        starts = starts_of(pair)
        tall = [jnp.concatenate([filtered(a * length + start) for a in range(radix)], axis=0) for start in starts]
        for start, y in zip(starts, left(outer_m, tall, False)):
            part = pl.ds(start, step)
            u_ref[:, part, :] = turned(y.reshape(radix, step, LANES), (t1_re[:, part, :], t1_im[:, part, :]))
        return carry

    take_own(0, rows, to_line)
    for group in range(GROUPS):
        take_group(0, group, to_line)
        if group:
            outer_in(lax.rem(me + n - group + 1, GROUPS), 0)
    outer_in(lax.rem(me + n - GROUPS + 1, GROUPS), 0)

    def inner_in(pair, carry):
        for i, y in enumerate(left(inner_m, [u_ref[2 * pair], u_ref[2 * pair + 1]], False)):
            z_ref[2 * pair + i] = turned(y, (t2_re[2 * pair + i], t2_im[2 * pair + i]))
        return carry

    def bins_of(t):
        return pl.ds(pl.multiple_of(t * SUB, SUB), SUB)

    half_rows, half_radix = rows // 2, radix // 2
    for h in range(2):
        lax.fori_loop(h * half_radix // 2, (h + 1) * half_radix // 2, inner_in, 0)
        towers = slice(h * half_radix, (h + 1) * half_radix)
        send_all(1 + h, half_rows, lambda t: z_ref[towers, bins_of(t), :].reshape(half_rows, LANES), 1.0)

    def half_copy(trip, c):
        part = pl.ds(pl.multiple_of(2 * c * SUB, 2 * SUB), 2 * SUB)
        return pltpu.make_async_remote_copy(
            src_ref=mine_ref.at[trip, :, part, :],
            dst_ref=theirs_ref.at[trip, :, part, :],
            send_sem=half_sent.at[trip, c],
            recv_sem=half_arrived.at[trip, c],
            device_id={"sub": 1 - parity},
            device_id_type=MESH,
        )

    def rows_forward(c, carry):
        parts = pair_of(c)
        for part, y in zip(parts, across(c, [x_ref[:, part, :] for part in parts], False)):
            mine_ref[0, :, part, :] = turned(y, (turn_re[...], turn_im[...]), True)
        half_copy(0, c).start()
        return carry

    def respond(c, carry):
        half_copy(0, c).wait_recv()
        for part in pair_of(c):
            both = theirs_ref[0, :, part, :] + sign * mine_ref[0, :, part, :]
            mine_ref[1, :, part, :] = turned(both, (resp_re[:, part, :], resp_im[:, part, :]))
        half_copy(1, c).start()
        return carry

    def rows_back(c, carry):
        half_copy(1, c).wait_recv()
        parts = pair_of(c)
        both = [theirs_ref[1, :, part, :] + sign * mine_ref[1, :, part, :] for part in parts]
        for part, y in zip(parts, across(c, [turned(x, (turn_re[...], turn_im[...])) for x in both], True)):
            v_ref[:, part, :] = y
        return carry

    for h in range(2):
        part = slice(h * half_rows, (h + 1) * half_rows)

        def row_in(t, x):
            x_ref[t, part, :] = turned(right(minus_m, x), (twist_re[t], twist_im[t]), True)

        take_all(1 + h, half_rows, row_in)
        for act in (rows_forward, respond, rows_back):
            lax.fori_loop(h * chunks // 2, (h + 1) * chunks // 2, act, 0)
        send_all(3 + h, half_rows, lambda t: row_out(t, part), 1.0)

    def inner_out(pair, carry):
        qs = (2 * pair, 2 * pair + 1)
        for q, y in zip(qs, left(inner_m, [turned(z_ref[q], (t2_re[q], t2_im[q]), True) for q in qs], True)):
            u_ref[q] = turned(y, (t1_re[q], t1_im[q]), True)
        return carry

    for h in range(2):
        towers = slice(h * half_radix, (h + 1) * half_radix)

        def to_bins(t, x):
            z_ref[towers, bins_of(t), :] = x.reshape(half_radix, SUB, LANES)

        take_all(3 + h, half_rows, to_bins)
        lax.fori_loop(h * half_radix // 2, (h + 1) * half_radix // 2, inner_out, 0)

    def outer_out(pair, carry):
        starts = starts_of(pair)
        got_back = left(outer_m, [u_ref[:, pl.ds(start, step), :].reshape(length, LANES) for start in starts], True)
        for start, y in zip(starts, got_back):
            for a in range(radix):
                line_ref[pl.ds(pl.multiple_of(a * length + start, step), step)] = y[a * step : (a + 1) * step]
        return carry

    def frames_of(t):
        return line_ref[pl.ds(pl.multiple_of(t * rows, SUB), rows)]

    for group in range(GROUPS):
        outer_out(lax.rem(me + group, GROUPS), 0)
        send_group(5, group, frames_of, norm_out)
    keep(5, rows, frames_of, norm_out)

    def to_out(t, x):
        out_ref[:, pl.ds(t, 1), :] = x.T[:, None, :]

    take_own(5, rows, to_out)
    for group in range(GROUPS):
        take_group(5, group, to_out)

    def finish(i):
        for trip, count in enumerate((rows, *[half_rows] * 4, rows)):
            for copy in copies(trip, i + 1, count):
                copy.wait_send()

    each(n - 1, finish)

    def finish_halves(c, carry):
        for trip in range(2):
            half_copy(trip, c).wait_send()
        return carry

    lax.fori_loop(0, chunks, finish_halves, 0)


def as_parts(matrix):
    hi = matrix.astype(bf16)
    lo = (matrix - hi.astype(np.float64)).astype(bf16)
    return jnp.asarray(hi), jnp.asarray(lo)


def roots(left_count, right_count, length, direction):
    product = np.arange(left_count)[:, None] * np.arange(right_count)[None, :] % length
    return np.exp(direction * 2j * np.pi * product / length)


def left_parts(length, copies):
    full = np.kron(roots(length, length, length, -1), np.eye(copies))
    return as_parts(np.concatenate([full.real, full.imag], axis=1))


def right_parts(length, direction):
    full = roots(length, length, length, direction)
    return as_parts(np.block([[full.real, full.imag], [-full.imag, full.real]]))


def lane_table(values):
    re, im = values.real, values.imag
    return (
        jnp.asarray(np.concatenate([re, re], axis=-1), f32),
        jnp.asarray(np.concatenate([-im, im], axis=-1), f32),
    )


def body(channels, synth_taps, chirp_phase):
    frames_dev, half = channels.shape[1:]
    n = lax.axis_size("tm")
    me = lax.axis_index("tm")
    parity = lax.axis_index("sub")
    frames = frames_dev * n
    series_len = frames * 2 * half
    radix, length = SUB, frames // SUB
    tap_count = synth_taps.shape[0]

    def partner(x):
        size = lax.axis_size("sub")
        return lax.ppermute(x, "sub", [(i, size - 1 - i) for i in range(size)])

    long_m = left_parts(n, SUB)
    outer_m = left_parts(radix, length // radix)
    inner_m = left_parts(length, 1)
    short_plus, short_minus = right_parts(WIDTH, 1), right_parts(WIDTH, -1)

    twist = lane_table(roots(n, WIDTH, half, 1)[:, None, :])
    turn = np.exp(1j * np.pi * np.arange(half) / half).reshape(n, 1, WIDTH)
    turns = lane_table(np.stack([np.ones_like(turn), turn]))
    taps = lax.dynamic_index_in_dim(synth_taps.reshape(tap_count, WIDTH, n), me, 2, keepdims=False)
    taps = jnp.concatenate([taps, taps], axis=-1)
    args = (
        channels, partner(channels), taps, chirp_phase, *turns, *twist, *long_m, *inner_m, *outer_m, *short_plus,
        *short_minus,
    )
    grid_shape, tower = (n, frames_dev, LANES), (radix, length, LANES)
    trips = 6
    out = pl.pallas_call(
        functools.partial(beam_kernel, 1.0 / math.sqrt(2 * half), 1.0 / series_len),
        out_shape=jax.ShapeDtypeStruct((LANES, n, frames_dev), f32),
        in_specs=[pl.BlockSpec(memory_space=pltpu.VMEM)] * len(args),
        out_specs=pl.BlockSpec(memory_space=pltpu.VMEM),
        scratch_shapes=[
            pltpu.VMEM(grid_shape, f32),
            pltpu.VMEM(grid_shape, f32),
            pltpu.VMEM(tower, f32),
            pltpu.VMEM(tower, f32),
            pltpu.VMEM((SUB + frames, LANES), f32),
            *[pltpu.VMEM(tower, f32)] * 4,
            *[pltpu.VMEM(grid_shape, f32)] * 2,
            pltpu.VMEM((2, *grid_shape), f32),
            pltpu.VMEM((2, *grid_shape), f32),
            pltpu.VMEM((trips, *grid_shape), bf16),
            pltpu.VMEM((trips, n, 1, LANES), f32),
            pltpu.VMEM((trips, *grid_shape), bf16),
            pltpu.VMEM((trips, n, 1, LANES), f32),
            *[pltpu.SemaphoreType.DMA((trips, n))] * 4,
            *[pltpu.SemaphoreType.DMA((2, frames_dev // (2 * SUB)))] * 2,
        ],
        compiler_params=pltpu.CompilerParams(collective_id=1, has_side_effects=True, vmem_limit_bytes=56 * 2**20),
        name="beam",
    )(*args)
    out = out.reshape(2, half, frames_dev).transpose(0, 2, 1)
    return out.reshape(2, frames_dev, 1, half)


def solution(mesh):
    placed = (P(None, ("beam", "tm"), "sub"), P(None, "sub", None), P("tm", "sub"))
    return jax.shard_map(
        body,
        mesh=mesh,
        in_specs=placed,
        out_specs=P(None, ("beam", "tm"), "sub", None),
        check_vma=False,
    )
```
